32 devices in a mesh: gx: 4 (over x, core), gy: 8 (over z, y).
Axes of the slice: x: 2, y: 2, z: 4, core: 2. Of those that a mesh axis runs over, the one named last changes fastest.
Arguments:
- atm_fields: bfloat16 [196608, 128], P(('gx', 'gy')), may hold values from -6 to 6
- atm_pos: int32 [768], replicated, may hold values from 0 to 767, as said below
- tile_src: int32 [5120], P(('gx', 'gy')), may hold values from 0 to 767, as said below
- tile_tgt: int32 [5120], P(('gx', 'gy')), may hold values from 0 to 1
- tile_count: int32 [32], P(('gx', 'gy')), may hold values from 128 to 160, as said below
- tile_weight: bfloat16 [5120, 256, 256], P(('gx', 'gy')), may hold values from -0.0625 to 0.0625
- ocean_state: bfloat16 [128, 128, 128], P('gy', 'gx'), may hold values from -6 to 6
- land_mask: int32 [128, 128], P('gy', 'gx'), may hold values 0 or 1
- mixing: float32 [128], replicated, may hold values from 0.03 to 0.24
Outputs:
- ocean_next: bfloat16 [128, 128, 128], P('gy', 'gx')
The draws below stay inside these ranges and needn't reach their ends.
Inputs may be any that keep to these rules, and one draw needn't show every extreme that they name: `atm_pos`: a permutation of the block positions. `tile_src`: among the 160 slots of one device, live or not, no owning device (atm_pos of the block // 24) is named by more than 8 slots; on every device with 160 live slots some owner is named by exactly 8. `tile_count`: live slots are a device's first ones; one device has exactly 160.
All inputs are finite; a program needn't handle non-finite values. No bound on the sum of `land_mask` on one device may be relied on, other than what follows from the above.
Results may differ from the reference program's by a relative error of at most 0.001.
Values may be sent and summed in bfloat16 or wider, within the bound.
A program may use at most 128 MiB of HBM per device.

```python
import math
import jax
import jax.numpy as jnp
from jax import lax

TILE_ROWS = 256
CHANNELS = 128
ATM_BLOCKS = 24
TILE_SLOTS = 160
LAT_CELLS = 16
LON_CELLS = 32
RECV_SLOTS = 256
TARGET_BLOCKS = 2
ALL_BLOCKS = 768
ALL_TILES = 5120
LATITUDES = 128
LONGITUDES = 128
N_GX = 4
N_GY = 8
DEVICES = 32


def block_order(key):
    return jax.random.permutation(jax.random.fold_in(key, 11), ATM_BLOCKS * DEVICES).astype(jnp.int32)


def draw_atm_pos(key, part):
    return block_order(key)


def draw_tile_src(key, part):
    ordering = block_order(key)
    inverse = jnp.argsort(ordering, stable=True).astype(jnp.int32)
    per_peer = RECV_SLOTS // DEVICES
    device_keys = jax.random.split(jax.random.fold_in(key, 23), DEVICES)

    def one_device(device_key):
        first_key, second_key, third_key = jax.random.split(device_key, 3)
        owner_table = jax.random.permutation(first_key, DEVICES).astype(jnp.int32)
        owners = owner_table[jnp.arange(TILE_SLOTS, dtype=jnp.int32) // per_peer]
        owners = jax.random.permutation(second_key, owners)
        local_slot = jax.random.randint(third_key, (TILE_SLOTS,), 0, ATM_BLOCKS, dtype=jnp.int32)
        return inverse[owners * ATM_BLOCKS + local_slot]
    return jax.vmap(one_device)(device_keys).reshape(DEVICES * TILE_SLOTS).astype(jnp.int32)


def draw_tile_count(key, part):
    first_key, second_key = jax.random.split(jax.random.fold_in(key, 37))
    lowest = TILE_SLOTS - TILE_SLOTS // 5
    counts = jax.random.randint(first_key, (DEVICES,), lowest, TILE_SLOTS + 1, dtype=jnp.int32)
    busiest = jax.random.randint(second_key, (), 0, DEVICES, dtype=jnp.int32)
    return jnp.where(jnp.arange(DEVICES, dtype=jnp.int32) == busiest, TILE_SLOTS, counts).astype(jnp.int32)


def with_ends(entries, stream_key, least, largest):
    index_at = [jax.random.randint(jax.random.fold_in(stream_key, axis), (), 0, length) for axis, length in enumerate(entries.shape)]
    main_axis = entries.shape.index(max(entries.shape))
    beside = index_at[:main_axis] + [(index_at[main_axis] + 1) % entries.shape[main_axis]] + index_at[main_axis + 1:]
    return entries.at[tuple(index_at)].set(least).at[tuple(beside)].set(largest)


def level_of(key, shape, cuts, smallest, high):
    level, own = 1.0, jax.random.fold_in(key, 6)
    for axis_at, blocks in cuts:
        draws = jnp.exp(jax.random.uniform(jax.random.fold_in(own, axis_at), (blocks,), jnp.float32, smallest / len(cuts), high / len(cuts)))
        level = level * jnp.repeat(draws, shape[axis_at] // blocks).reshape([-1 if axis == axis_at else 1 for axis in range(len(shape))])
    return level


def bell_draw(stream_key, extent, width, bound, cuts=(), kind=jnp.bfloat16):
    entries = jax.random.normal(stream_key, extent, jnp.float32) * width
    if len(cuts) > 0:
        entries = level_of(stream_key, extent, cuts, -0.22, 0.18) * entries
    return jnp.clip(entries, min=-bound, max=bound).astype(kind)


def setup_inputs(seed: int = 0) -> dict:
    arg_keys = jax.random.split(jax.random.key(seed), 10)
    return {
        "atm_fields": bell_draw(arg_keys[0], (ALL_BLOCKS * TILE_ROWS, CHANNELS), 1.0, 6.0, ((0, 32),)),
        "atm_pos": draw_atm_pos(jax.random.fold_in(arg_keys[9], 71), 0),
        "tile_src": draw_tile_src(jax.random.fold_in(arg_keys[9], 71), 0),
        "tile_tgt": with_ends(jax.random.randint(arg_keys[3], (ALL_TILES,), 0, TARGET_BLOCKS), jax.random.fold_in(arg_keys[3], 1), 0, TARGET_BLOCKS - 1).astype(jnp.int32),
        "tile_count": draw_tile_count(jax.random.fold_in(arg_keys[9], 71), 0),
        "tile_weight": bell_draw(arg_keys[5], (ALL_TILES, TILE_ROWS, TILE_ROWS), (TILE_ROWS * TILE_SLOTS // 4) ** -0.5, 0.0625, ((0, 32),)),
        "ocean_state": bell_draw(arg_keys[6], (LATITUDES, LONGITUDES, CHANNELS), 1.0, 6.0, ((0, 8), (1, 4))),
        "land_mask": with_ends((jax.random.randint(arg_keys[7], (LATITUDES, LONGITUDES), 0, 4) < 3).astype(jnp.int32), jax.random.fold_in(arg_keys[7], 1), 0, 1),
        "mixing": jnp.clip(jnp.exp(jax.random.uniform(arg_keys[8], (CHANNELS,), jnp.float32, math.log(0.03), math.log(0.24))), 0.03, 0.24),
    }


def neighbours(field):
    west_side = jnp.roll(field, 1, axis=1)
    east_side = jnp.roll(field, -1, axis=1)
    south_side = jnp.concatenate([jnp.zeros_like(field[:1]), field[:-1]], axis=0)
    north_side = jnp.concatenate([field[1:], jnp.flip(field[-1:], axis=1)], axis=0)
    return (west_side, east_side, south_side, north_side)


def reference(atm_fields, atm_pos, tile_src, tile_tgt, tile_count, tile_weight, ocean_state, land_mask, mixing):
    devices = N_GX * N_GY
    block_table = atm_fields.reshape(ATM_BLOCKS * devices, TILE_ROWS, CHANNELS)

    def remap_device(pieces):
        weights, sources, targets, tile_live = pieces
        gathered = block_table[atm_pos[sources]].astype(jnp.float32)
        partial_sum = jnp.einsum("tij,tjc->tic", weights.astype(jnp.float32), gathered, precision=lax.Precision.HIGHEST)
        active = jnp.arange(TILE_SLOTS, dtype=jnp.int32) < tile_live
        select = ((targets[:, None] == jnp.arange(TARGET_BLOCKS, dtype=jnp.int32)[None, :]) & active[:, None]).astype(jnp.float32)
        summed = jnp.einsum("tb,tic->bic", select, partial_sum, precision=lax.Precision.HIGHEST)
        return summed.reshape(LAT_CELLS, LON_CELLS, CHANNELS)

    remapped = lax.map(remap_device, (tile_weight.reshape(devices, TILE_SLOTS, TILE_ROWS, TILE_ROWS), tile_src.reshape(devices, TILE_SLOTS), tile_tgt.reshape(devices, TILE_SLOTS), tile_count))
    forcing = remapped.reshape(N_GX, N_GY, LAT_CELLS, LON_CELLS, CHANNELS).transpose(1, 2, 0, 3, 4)
    forcing = forcing.reshape(N_GY * LAT_CELLS, N_GX * LON_CELLS, CHANNELS)
    center = ocean_state.astype(jnp.float32)
    wet_mask = land_mask.astype(jnp.float32)
    diffusion = jnp.zeros_like(center)
    for side_state, side_mask in zip(neighbours(center), neighbours(wet_mask)):
        diffusion = diffusion + side_mask[..., None] * (side_state - center)
    result = wet_mask[..., None] * (center + forcing + mixing * diffusion)
    return result.astype(jnp.bfloat16)
```

```python
import functools

import jax
import jax.numpy as jnp
from jax import lax
from jax.experimental import pallas as pl
from jax.experimental.pallas import tpu as pltpu
from jax.sharding import PartitionSpec as P

RECV_SLOTS = 256
GATHER_BYTES = 64 * 2**20
MESH = pl.DeviceIdType.MESH
LOOKAHEAD = 10.0
D2D_SPEED = 10.0


def row_parts(rows):
    unit = 32
    b_rows = rows * 2 // 9 // unit * unit
    a_half = (rows - b_rows) // 2 // 16 * 16
    return {
        "B0": (0, b_rows // 2),
        "B1": (b_rows // 2, b_rows - b_rows // 2),
        "BF": (0, b_rows),
        "A0": (b_rows, a_half),
        "A1": (b_rows + a_half, rows - b_rows - a_half),
        "all": (0, rows),
    }


def pieces_of(part):
    return {"BF": ("B0", "B1"), "all": ("B0", "B1", "A0", "A1")}.get(part, (part,))


def schedule(depth, parts, rows):
    flip = {
        "x": {"o": "x", "y": "d", "x": "o", "d": "y"},
        "y": {"o": "y", "x": "d", "y": "o", "d": "x"},
    }
    messages = []
    for z in range(depth):
        for oz in range(depth):
            far = abs(oz - z)
            for part in ("A0", "A1"):
                for queue in ("x", "y"):
                    messages.append((z, queue, "o", oz, part, 2 * far + 1))
            messages.append((z, "x", "y", oz, "A1", 2 * far + 4))
            messages.append((z, "y", "x", oz, "A0", 2 * far + 4))
            for queue, step in (("up", 1), ("down", -1)):
                if 0 <= z + step < depth and (oz - z) * step <= 0:
                    for part in ("A0", "A1"):
                        messages.append((z, queue, "o", oz, part, far))
                    for across in ("o", "x", "y", "d"):
                        messages.append((z, queue, across, oz, "BF", 100 + far))
            for across in ("o", "x", "y", "d"):
                if (across, oz) == ("o", z):
                    messages.append((z, "pair", across, oz, "all", 0))
                else:
                    for part in ("BF", "A0", "A1"):
                        messages.append((z, "pair", across, oz, part, far))
        for queue in ("x", "y"):
            for part in ("B0", "B1"):
                messages.append((z, queue, "o", z, part, 0))
        messages.append((z, "x", "y", z, "B1", 2))
        messages.append((z, "y", "x", z, "B0", 2))

    arrived = {(z, "o", z, p): (0.0, None) for z in range(depth) for p in ("B0", "B1", "A0", "A1")}
    free = {}
    waiting = list(messages)
    issued = []
    while waiting:
        best = None
        for message in waiting:
            z, queue, across, oz, part, rank = message
            needs = [arrived.get((z, across, oz, p)) for p in pieces_of(part)]
            if any(n is None for n in needs):
                continue
            ready = max(n[0] for n in needs)
            start = max(ready, free.get((z, queue), 0.0))
            key = (start, rank, messages.index(message))
            if best is None or key < best[0]:
                best = (key, message, ready, start)
        _, message, ready, start = best
        waiting.remove(message)
        z, queue, across, oz, part, rank = message
        length = parts[part][1] / 256 / (D2D_SPEED if queue == "pair" else 1.0)
        end = start + length
        free[(z, queue)] = end
        if queue != "pair":
            to = z + {"up": 1, "down": -1}.get(queue, 0)
            landed = flip[queue][across] if queue in flip else across
            for p in pieces_of(part):
                arrived[(to, landed, oz, p)] = (end + 1.5, (landed, oz, part))
        issued.append((max(ready, start - LOOKAHEAD), start, z, message))
    plans = []
    for z in range(depth):
        mine = sorted((i for i in issued if i[2] == z), key=lambda i: i[:2])
        plan = []
        for _, _, _, message in mine:
            _, queue, across, oz, part, _ = message
            needs = []
            for p in pieces_of(part):
                via = arrived[(z, across, oz, p)][1]
                if via is not None and via not in needs:
                    needs.append(via)
            plan.append((queue, across, oz, part, tuple(needs), None if queue == "pair" else flip.get(queue, {}).get(across, across)))
        plans.append(plan)
    return plans


def gather_kernel(
    sizes, plans, parts, recv_index, pair_index, fields, lon, lat, out, lon_out, lat_out,
    stage, send_sem, recv_sem, pair_sem, local_sem, halo_send, halo_recv,
):
    n_gx, n_gy = sizes
    gx, gy = lax.axis_index("gx"), lax.axis_index("gy")
    rows = fields.shape[0]
    core, y, z = gx % 2, gy % 2, gy // 2
    across_x = (gx + 2) % n_gx
    across_y = gy + 1 - 2 * y
    other_core = gx + 1 - 2 * core
    right, left = (gx + 1) % n_gx, (gx + n_gx - 1) % n_gx
    north, south = (gy + 1) % n_gy, (gy + n_gy - 1) % n_gy
    mirror = n_gx - 1 - gx
    above, below = (gy + 2) % n_gy, (gy + n_gy - 2) % n_gy

    barrier = pltpu.get_barrier_semaphore()
    greeted = [
        (across_x, gy), (gx, across_y), (other_core, gy), (gx, above), (gx, below),
        (right, gy), (left, gy), (gx, north), (gx, south), (mirror, gy),
    ]
    for device in greeted:
        pl.semaphore_signal(barrier, inc=1, device_id=device, device_id_type=MESH)
    pl.semaphore_wait(barrier, len(greeted))

    take = pltpu.make_async_copy(fields, stage, local_sem.at[0])
    take.start()

    halo = []
    for i, (source, target, device) in enumerate((
        (lon.at[1], lon_out.at[0], (right, gy)),
        (lon.at[0], lon_out.at[1], (left, gy)),
        (lat.at[1], lat_out.at[0], (gx, north)),
        (lat.at[0], lat_out.at[1], (gx, south)),
        (lat.at[2], lat_out.at[2], (mirror, gy)),
    )):
        halo.append(pltpu.make_async_remote_copy(
            src_ref=source, dst_ref=target, send_sem=halo_send.at[i], recv_sem=halo_recv.at[i],
            device_id=device, device_id_type=MESH,
        ))
        halo[-1].start()

    def first_row(across, oz):
        ox = across_x if across in ("x", "d") else gx
        oy = 1 - y if across in ("y", "d") else y
        return (ox * n_gy + oz * 2 + oy) * rows

    def region(ref, across, oz, part):
        offset, length = parts[part]
        return ref.at[pl.ds(pl.multiple_of(first_row(across, oz) + offset, 16), length)]

    targets = {
        "x": (across_x, gy), "y": (gx, across_y), "pair": (other_core, gy),
        "up": (gx, above), "down": (gx, below),
    }

    def copy_of(here, entry, slot):
        queue, across, oz, part, _, landed = entry
        if (across, oz) == ("o", here):
            offset, length = parts[part]
            source = fields.at[pl.ds(offset, length)]
        else:
            source = region(out, across, oz, part)
        if queue == "pair":
            semaphore = pair_sem.at[pair_index[(across, oz, part)]]
        else:
            semaphore = recv_sem.at[recv_index[(landed, oz, part)]]
        return pltpu.make_async_remote_copy(
            src_ref=source, dst_ref=region(out, across, oz, part), send_sem=send_sem.at[slot],
            recv_sem=semaphore, device_id=targets[queue], device_id_type=MESH,
        )

    def arrival(across, oz, part, semaphore):
        place = region(out, across, oz, part)
        return pltpu.make_async_copy(place, place, semaphore)

    def arrival_pair(oz_across, oz, part):
        offset, length = parts[part]
        ox = {"x": (other_core + 2) % n_gx, "d": (other_core + 2) % n_gx}.get(oz_across, other_core)
        oy = 1 - y if oz_across in ("y", "d") else y
        start = (ox * n_gy + oz * 2 + oy) * rows + offset
        place = out.at[pl.ds(pl.multiple_of(start, 16), length)]
        return pltpu.make_async_copy(place, place, pair_sem.at[pair_index[(oz_across, oz, part)]])

    def run(here, plan):
        seen = set()
        started = []
        put = None
        for slot, entry in enumerate(plan):
            for need in entry[4]:
                if need not in seen:
                    seen.add(need)
                    arrival(*need, recv_sem.at[recv_index[need]]).wait()
            copy = copy_of(here, entry, slot)
            copy.start()
            started.append(copy)
            if slot == 8:
                take.wait()
                put = pltpu.make_async_copy(stage, region(out, "o", here, "all"), local_sem.at[1])
                put.start()
        put.wait()
        for copy in started:
            copy.wait_send()
        for entry in plan:
            if entry[0] == "pair":
                arrival_pair(entry[1], entry[2], entry[3]).wait()

    for here, plan in enumerate(plans):
        pl.when(z == here)(functools.partial(run, here, plan))
    for copy in halo:
        copy.wait()


def gather_all(fields, lon, lat, sizes):
    n_gx, n_gy = sizes
    rows, channels = fields.shape
    depth = n_gy // 2
    parts = row_parts(rows)
    plans = schedule(depth, parts, rows)
    recv_index, pair_index = {}, {}
    for here, plan in enumerate(plans):
        for queue, across, oz, part, needs, landed in plan:
            if queue == "pair":
                pair_index.setdefault((across, oz, part), len(pair_index))
            else:
                recv_index.setdefault((landed, oz, part), len(recv_index))
    slots = max(len(plan) for plan in plans)
    any_space = pl.BlockSpec(memory_space=pl.ANY)
    vmem = pl.BlockSpec(memory_space=pltpu.VMEM)
    return pl.pallas_call(
        functools.partial(gather_kernel, sizes, plans, parts, recv_index, pair_index),
        out_shape=(
            jax.ShapeDtypeStruct((rows * n_gx * n_gy, channels), fields.dtype),
            jax.ShapeDtypeStruct(lon.shape, lon.dtype),
            jax.ShapeDtypeStruct(lat.shape, lat.dtype),
        ),
        in_specs=[any_space, any_space, any_space],
        out_specs=(any_space, any_space, any_space),
        scratch_shapes=[
            pltpu.VMEM((rows, channels), fields.dtype),
            pltpu.SemaphoreType.DMA((slots,)),
            pltpu.SemaphoreType.DMA((len(recv_index),)),
            pltpu.SemaphoreType.DMA((len(pair_index),)),
            pltpu.SemaphoreType.DMA((2,)),
            pltpu.SemaphoreType.DMA((5,)),
            pltpu.SemaphoreType.DMA((5,)),
        ],
        compiler_params=pltpu.CompilerParams(
            collective_id=0, has_side_effects=True, vmem_limit_bytes=8 * 2**20
        ),
        name="gather_fields",
    )(fields, lon, lat)


def remap_kernel(
    per_step, block_of, targets, meta, weights, *refs,
):
    blocks = refs[:per_step]
    state, mask, mixing, lon, lat, out, total = refs[per_step:]
    step = pl.program_id(0)
    lat_rows, lon_cols, channels = state.shape

    @pl.when(step == 0)
    def _():
        center = state[...].astype(jnp.float32)
        wet = mask[...].astype(jnp.float32)
        west, east = lon[0].astype(jnp.float32), lon[1].astype(jnp.float32)
        top = (meta[1] != 0).astype(jnp.float32)
        inner_south = (meta[2] == 0).astype(jnp.float32)
        south = lat[0].astype(jnp.float32)
        north = lat[1].astype(jnp.float32) * (1.0 - top) + lat[2].astype(jnp.float32) * top
        south_mask = south[1] * inner_south
        sides = (
            (
                jnp.concatenate([west[0][:, None], center[:, :-1]], axis=1),
                jnp.concatenate([west[1][:, None], wet[:, :-1]], axis=1),
            ),
            (
                jnp.concatenate([center[:, 1:], east[0][:, None]], axis=1),
                jnp.concatenate([wet[:, 1:], east[1][:, None]], axis=1),
            ),
            (
                jnp.concatenate([south[0][None], center[:-1]], axis=0),
                jnp.concatenate([south_mask[None], wet[:-1]], axis=0),
            ),
            (
                jnp.concatenate([center[1:], north[0][None]], axis=0),
                jnp.concatenate([wet[1:], north[1][None]], axis=0),
            ),
        )
        diffusion = jnp.zeros_like(center)
        for side_state, side_mask in sides:
            diffusion = diffusion + side_mask * (side_state - center)
        start = center + mixing[...][0][None, None, :] * diffusion
        total[...] = start.reshape(total.shape)

    for k in range(per_step):
        tile = step * per_step + k

        @pl.when(tile < meta[0])
        def _():
            product = jnp.dot(weights[k], blocks[k][...], preferred_element_type=jnp.float32)
            total[targets[tile]] += product

    @pl.when(step == pl.num_programs(0) - 1)
    def _():
        wet = mask[...].astype(jnp.float32)
        out[...] = (wet * total[...].reshape(out.shape)).astype(out.dtype)


def remap(table, block_of, tile_tgt, meta, tile_weight, state, mask, mixing, lon, lat):
    tiles, block_rows, _ = tile_weight.shape
    channels = table.shape[1]
    cells = state.shape[0] * state.shape[1]
    per_step = max(d for d in range(1, 17) if tiles % d == 0)

    def block_spec(k):
        def index(i, block_of, tile_tgt, meta):
            return (block_of[i * per_step + k], 0)

        return pl.BlockSpec((block_rows, channels), index)

    def whole(array):
        return pl.BlockSpec(array.shape, lambda i, *_: (0,) * array.ndim)

    mixing = mixing[None]
    rest = (state, mask, mixing, lon, lat)
    return pl.pallas_call(
        functools.partial(remap_kernel, per_step),
        grid_spec=pltpu.PrefetchScalarGridSpec(
            num_scalar_prefetch=3,
            grid=(tiles // per_step,),
            in_specs=[
                pl.BlockSpec((per_step, block_rows, block_rows), lambda i, *_: (i, 0, 0)),
                *[block_spec(k) for k in range(per_step)],
                *[whole(a) for a in rest],
            ],
            out_specs=whole(state),
            scratch_shapes=[pltpu.VMEM((cells // block_rows, block_rows, channels), jnp.float32)],
        ),
        out_shape=jax.ShapeDtypeStruct(state.shape, state.dtype),
        compiler_params=pltpu.CompilerParams(
            dimension_semantics=("arbitrary",), vmem_limit_bytes=48 * 2**20
        ),
        name="remap_step",
    )(block_of, tile_tgt, meta, tile_weight, *[table] * per_step, *rest)


def exchange(atm_fields, positions, tile_live, block_rows):
    channels = atm_fields.shape[1]
    block_count = atm_fields.shape[0] // block_rows
    devices = lax.axis_size("gx") * lax.axis_size("gy")
    per_peer = RECV_SLOTS // devices
    owners = positions // block_count
    local_slot = positions % block_count
    ordinal = jnp.arange(positions.shape[0], dtype=jnp.int32)
    active = ordinal < tile_live
    earlier = (
        (owners[:, None] == owners[None, :])
        & active[None, :]
        & (ordinal[None, :] < ordinal[:, None])
    )
    wanted_slot = owners * per_peer + jnp.sum(earlier.astype(jnp.int32), axis=1)
    slots_flat = jnp.arange(RECV_SLOTS, dtype=jnp.int32)
    matches = (wanted_slot[None, :] == slots_flat[:, None]) & active[None, :]
    asking = jnp.sum(jnp.where(matches, local_slot[None, :], 0), axis=1)
    wanted = lax.all_to_all(
        asking.reshape(devices, per_peer), ("gx", "gy"), split_axis=0, concat_axis=0, tiled=True
    ).reshape(RECV_SLOTS)
    outgoing = atm_fields.reshape(block_count, block_rows, channels)[wanted]
    outgoing = outgoing.reshape(devices, per_peer, block_rows, channels)
    arrived = lax.all_to_all(outgoing, ("gx", "gy"), split_axis=0, concat_axis=0, tiled=True)
    return arrived.reshape(RECV_SLOTS * block_rows, channels), jnp.where(active, wanted_slot, 0)


def swap_edges(lon, lat, sizes):
    n_gx, n_gy = sizes

    def shift(value, axis, size, by):
        return lax.ppermute(value, axis, [(i, (i + by) % size) for i in range(size)])

    lon_out = jnp.stack([shift(lon[1], "gx", n_gx, 1), shift(lon[0], "gx", n_gx, -1)])
    fold = lax.ppermute(lat[2], "gx", [(i, n_gx - 1 - i) for i in range(n_gx)])
    lat_out = jnp.stack([shift(lat[1], "gy", n_gy, 1), shift(lat[0], "gy", n_gy, -1), fold])
    return lon_out, lat_out


def local(
    atm_fields, atm_pos, tile_src, tile_tgt, tile_count, tile_weight, ocean_state, land_mask, mixing
):
    sizes = (lax.axis_size("gx"), lax.axis_size("gy"))
    block_rows = tile_weight.shape[1]
    positions = atm_pos[tile_src]
    mask = jnp.broadcast_to(land_mask.astype(jnp.bfloat16)[..., None], ocean_state.shape)
    both = jnp.stack([ocean_state, mask])
    lon = jnp.stack([both[:, :, 0], both[:, :, -1]])
    lat = jnp.stack([both[:, 0], both[:, -1], jnp.flip(both[:, -1], 1)])
    row = lax.axis_index("gy")
    meta = jnp.stack([
        tile_count[0], (row == sizes[1] - 1).astype(jnp.int32), (row == 0).astype(jnp.int32)
    ])
    fits = atm_fields.size * 2 * sizes[0] * sizes[1] <= GATHER_BYTES
    if fits and sizes[0] == 4 and sizes[1] % 2 == 0:
        table, lon_in, lat_in = gather_all(atm_fields, lon, lat, sizes)
        block_of = positions
    else:
        table, block_of = exchange(atm_fields, positions, tile_count[0], block_rows)
        lon_in, lat_in = swap_edges(lon, lat, sizes)
    return remap(
        table, block_of, tile_tgt, meta, tile_weight, ocean_state, mask, mixing, lon_in, lat_in
    )


def solution(mesh):
    in_specs = (
        P(("gx", "gy"), None),
        P(),
        P(("gx", "gy")),
        P(("gx", "gy")),
        P(("gx", "gy")),
        P(("gx", "gy"), None, None),
        P("gy", "gx", None),
        P("gy", "gx"),
        P(),
    )
    out_specs = P("gy", "gx", None)
    return jax.shard_map(local, mesh=mesh, in_specs=in_specs, out_specs=out_specs, check_vma=False)
```

```python
import functools

import jax
import jax.numpy as jnp
from jax import lax
from jax.experimental import pallas as pl
from jax.experimental.pallas import tpu as pltpu
from jax.sharding import PartitionSpec as P

RECV_SLOTS = 256
GATHER_BYTES = 64 * 2**20
VMEM_BYTES = 67043328
MESH = pl.DeviceIdType.MESH
LOOKAHEAD = 10.0
D2D_SPEED = 10.0


def row_parts(rows):
    unit = 32
    b_rows = rows * 2 // 9 // unit * unit
    a_half = (rows - b_rows) // 2 // 16 * 16
    return {
        "B0": (0, b_rows // 2),
        "B1": (b_rows // 2, b_rows - b_rows // 2),
        "BF": (0, b_rows),
        "A0": (b_rows, a_half),
        "A1": (b_rows + a_half, rows - b_rows - a_half),
        "all": (0, rows),
    }


def pieces_of(part):
    return {"BF": ("B0", "B1"), "all": ("B0", "B1", "A0", "A1")}.get(part, (part,))


def schedule(depth, parts, rows):
    flip = {
        "x": {"o": "x", "y": "d", "x": "o", "d": "y"},
        "y": {"o": "y", "x": "d", "y": "o", "d": "x"},
    }
    messages = []
    for z in range(depth):
        for oz in range(depth):
            far = abs(oz - z)
            for part in ("A0", "A1"):
                for queue in ("x", "y"):
                    messages.append((z, queue, "o", oz, part, 2 * far + 1))
            messages.append((z, "x", "y", oz, "A1", 2 * far + 4))
            messages.append((z, "y", "x", oz, "A0", 2 * far + 4))
            for queue, step in (("up", 1), ("down", -1)):
                if 0 <= z + step < depth and (oz - z) * step <= 0:
                    for part in ("A0", "A1"):
                        messages.append((z, queue, "o", oz, part, far))
                    for across in ("o", "x", "y", "d"):
                        messages.append((z, queue, across, oz, "BF", 100 + far))
            for across in ("o", "x", "y", "d"):
                if (across, oz) == ("o", z):
                    messages.append((z, "pair", across, oz, "all", 0))
                else:
                    for part in ("BF", "A0", "A1"):
                        messages.append((z, "pair", across, oz, part, far))
        for queue in ("x", "y"):
            for part in ("B0", "B1"):
                messages.append((z, queue, "o", z, part, 0))
        messages.append((z, "x", "y", z, "B1", 2))
        messages.append((z, "y", "x", z, "B0", 2))

    arrived = {(z, "o", z, p): (0.0, None) for z in range(depth) for p in ("B0", "B1", "A0", "A1")}
    free = {}
    waiting = list(messages)
    issued = []
    while waiting:
        best = None
        for message in waiting:
            z, queue, across, oz, part, rank = message
            needs = [arrived.get((z, across, oz, p)) for p in pieces_of(part)]
            if any(n is None for n in needs):
                continue
            ready = max(n[0] for n in needs)
            start = max(ready, free.get((z, queue), 0.0))
            key = (start, rank, messages.index(message))
            if best is None or key < best[0]:
                best = (key, message, ready, start)
        _, message, ready, start = best
        waiting.remove(message)
        z, queue, across, oz, part, rank = message
        length = parts[part][1] / 256 / (D2D_SPEED if queue == "pair" else 1.0)
        end = start + length
        free[(z, queue)] = end
        if queue != "pair":
            to = z + {"up": 1, "down": -1}.get(queue, 0)
            landed = flip[queue][across] if queue in flip else across
            for p in pieces_of(part):
                arrived[(to, landed, oz, p)] = (end + 1.5, (landed, oz, part))
        issued.append((max(ready, start - LOOKAHEAD), start, z, message))
    plans = []
    for z in range(depth):
        mine = sorted((i for i in issued if i[2] == z), key=lambda i: i[:2])
        plan = []
        for _, _, _, message in mine:
            _, queue, across, oz, part, _ = message
            needs = []
            for p in pieces_of(part):
                via = arrived[(z, across, oz, p)][1]
                if via is not None and via not in needs:
                    needs.append(via)
            plan.append((queue, across, oz, part, tuple(needs), None if queue == "pair" else flip.get(queue, {}).get(across, across)))
        plans.append(plan)
    return plans


def gather_kernel(
    sizes, plans, parts, recv_index, pair_index, fields, lon, lat, weights, out, lon_out, lat_out,
    weights_out,
    stage, send_sem, recv_sem, pair_sem, local_sem, halo_send, halo_recv,
):
    n_gx, n_gy = sizes
    gx, gy = lax.axis_index("gx"), lax.axis_index("gy")
    rows = fields.shape[0]
    core, y, z = gx % 2, gy % 2, gy // 2
    across_x = (gx + 2) % n_gx
    across_y = gy + 1 - 2 * y
    other_core = gx + 1 - 2 * core
    right, left = (gx + 1) % n_gx, (gx + n_gx - 1) % n_gx
    north, south = (gy + 1) % n_gy, (gy + n_gy - 1) % n_gy
    mirror = n_gx - 1 - gx
    above, below = (gy + 2) % n_gy, (gy + n_gy - 2) % n_gy

    barrier = pltpu.get_barrier_semaphore()
    greeted = [
        (across_x, gy), (gx, across_y), (other_core, gy), (gx, above), (gx, below),
        (right, gy), (left, gy), (gx, north), (gx, south), (mirror, gy),
    ]
    for device in greeted:
        pl.semaphore_signal(barrier, inc=1, device_id=device, device_id_type=MESH)
    pl.semaphore_wait(barrier, len(greeted))

    take = pltpu.make_async_copy(fields, stage, local_sem.at[0])
    take.start()
    near = pltpu.make_async_copy(weights, weights_out, local_sem.at[2])
    near.start()

    halo = []
    for i, (source, target, device) in enumerate((
        (lon.at[1], lon_out.at[0], (right, gy)),
        (lon.at[0], lon_out.at[1], (left, gy)),
        (lat.at[1], lat_out.at[0], (gx, north)),
        (lat.at[0], lat_out.at[1], (gx, south)),
        (lat.at[2], lat_out.at[2], (mirror, gy)),
    )):
        halo.append(pltpu.make_async_remote_copy(
            src_ref=source, dst_ref=target, send_sem=halo_send.at[i], recv_sem=halo_recv.at[i],
            device_id=device, device_id_type=MESH,
        ))
        halo[-1].start()

    def first_row(across, oz):
        ox = across_x if across in ("x", "d") else gx
        oy = 1 - y if across in ("y", "d") else y
        return (ox * n_gy + oz * 2 + oy) * rows

    def region(ref, across, oz, part):
        offset, length = parts[part]
        return ref.at[pl.ds(pl.multiple_of(first_row(across, oz) + offset, 16), length)]

    targets = {
        "x": (across_x, gy), "y": (gx, across_y), "pair": (other_core, gy),
        "up": (gx, above), "down": (gx, below),
    }

    def copy_of(here, entry, slot):
        queue, across, oz, part, _, landed = entry
        if (across, oz) == ("o", here):
            offset, length = parts[part]
            source = fields.at[pl.ds(offset, length)]
        else:
            source = region(out, across, oz, part)
        if queue == "pair":
            semaphore = pair_sem.at[pair_index[(across, oz, part)]]
        else:
            semaphore = recv_sem.at[recv_index[(landed, oz, part)]]
        return pltpu.make_async_remote_copy(
            src_ref=source, dst_ref=region(out, across, oz, part), send_sem=send_sem.at[slot],
            recv_sem=semaphore, device_id=targets[queue], device_id_type=MESH,
        )

    def arrival(across, oz, part, semaphore):
        place = region(out, across, oz, part)
        return pltpu.make_async_copy(place, place, semaphore)

    def arrival_pair(oz_across, oz, part):
        offset, length = parts[part]
        ox = {"x": (other_core + 2) % n_gx, "d": (other_core + 2) % n_gx}.get(oz_across, other_core)
        oy = 1 - y if oz_across in ("y", "d") else y
        start = (ox * n_gy + oz * 2 + oy) * rows + offset
        place = out.at[pl.ds(pl.multiple_of(start, 16), length)]
        return pltpu.make_async_copy(place, place, pair_sem.at[pair_index[(oz_across, oz, part)]])

    def run(here, plan):
        seen = set()
        started = []
        put = None
        for slot, entry in enumerate(plan):
            for need in entry[4]:
                if need not in seen:
                    seen.add(need)
                    arrival(*need, recv_sem.at[recv_index[need]]).wait()
            copy = copy_of(here, entry, slot)
            copy.start()
            started.append(copy)
            if slot == 8:
                take.wait()
                put = pltpu.make_async_copy(stage, region(out, "o", here, "all"), local_sem.at[1])
                put.start()
        put.wait()
        for copy in started:
            copy.wait_send()
        for entry in plan:
            if entry[0] == "pair":
                arrival_pair(entry[1], entry[2], entry[3]).wait()

    for here, plan in enumerate(plans):
        pl.when(z == here)(functools.partial(run, here, plan))
    for copy in halo:
        copy.wait()
    near.wait()


def gather_all(fields, lon, lat, weights, sizes):
    n_gx, n_gy = sizes
    rows, channels = fields.shape
    depth = n_gy // 2
    parts = row_parts(rows)
    plans = schedule(depth, parts, rows)
    recv_index, pair_index = {}, {}
    for here, plan in enumerate(plans):
        for queue, across, oz, part, needs, landed in plan:
            if queue == "pair":
                pair_index.setdefault((across, oz, part), len(pair_index))
            else:
                recv_index.setdefault((landed, oz, part), len(recv_index))
    slots = max(len(plan) for plan in plans)
    grant = max(VMEM_BYTES - weights.size * 2 - 12 * 2**20, 8 * 2**20)
    any_space = pl.BlockSpec(memory_space=pl.ANY)
    hbm = pl.BlockSpec(memory_space=pltpu.HBM)
    return pl.pallas_call(
        functools.partial(gather_kernel, sizes, plans, parts, recv_index, pair_index),
        out_shape=(
            jax.ShapeDtypeStruct((rows * n_gx * n_gy, channels), fields.dtype),
            jax.ShapeDtypeStruct(lon.shape, lon.dtype),
            jax.ShapeDtypeStruct(lat.shape, lat.dtype),
            jax.ShapeDtypeStruct(weights.shape, weights.dtype),
        ),
        in_specs=[hbm, any_space, any_space, hbm],
        out_specs=(hbm, any_space, any_space, any_space),
        scratch_shapes=[
            pltpu.VMEM((rows, channels), fields.dtype),
            pltpu.SemaphoreType.DMA((slots,)),
            pltpu.SemaphoreType.DMA((len(recv_index),)),
            pltpu.SemaphoreType.DMA((len(pair_index),)),
            pltpu.SemaphoreType.DMA((3,)),
            pltpu.SemaphoreType.DMA((5,)),
            pltpu.SemaphoreType.DMA((5,)),
        ],
        compiler_params=pltpu.CompilerParams(
            collective_id=0, has_side_effects=True, vmem_limit_bytes=grant
        ),
        cost_estimate=pl.CostEstimate(
            flops=0, transcendentals=0, bytes_accessed=10 * rows * channels * 2 * n_gx * n_gy
        ),
        name="gather_fields",
    )(fields, lon, lat, weights)


def remap_kernel(
    per_step, place_of, source, targets, live, weights, *refs,
):
    blocks = refs[:per_step]
    state, mask, mixing, lon, lat, out, base, total = refs[per_step:]
    step = pl.program_id(0)
    lat_rows, lon_cols, channels = state.shape
    block_rows = weights.shape[1]
    target_blocks = total.shape[1] // channels

    columns = []
    for k in range(per_step):
        tile = step * per_step + k
        target = jnp.where(tile < live[0], targets[tile], -1)
        block = blocks[k][...]
        columns.append(jnp.concatenate(
            [jnp.where(target == b, block, jnp.zeros_like(block)) for b in range(target_blocks)],
            axis=1,
        ))
    product = jnp.dot(
        jnp.concatenate([weights[k] for k in range(per_step)], axis=1),
        jnp.concatenate(columns, axis=0),
        preferred_element_type=jnp.float32,
    )

    @pl.when(step == 0)
    def _():
        center = state[...].astype(jnp.float32)
        wet = mask[...].astype(jnp.float32)
        row = lax.axis_index("gy")
        top = (row == lax.axis_size("gy") - 1).astype(jnp.float32)
        inner_south = (row != 0).astype(jnp.float32)
        west, east = lon[0].astype(jnp.float32), lon[1].astype(jnp.float32)
        south = lat[0].astype(jnp.float32)
        north = lat[1].astype(jnp.float32) * (1.0 - top) + lat[2].astype(jnp.float32) * top
        south_mask = south[1] * inner_south
        sides = (
            (
                jnp.concatenate([west[0][:, None], center[:, :-1]], axis=1),
                jnp.concatenate([west[1][:, None], wet[:, :-1]], axis=1),
            ),
            (
                jnp.concatenate([center[:, 1:], east[0][:, None]], axis=1),
                jnp.concatenate([wet[:, 1:], east[1][:, None]], axis=1),
            ),
            (
                jnp.concatenate([south[0][None], center[:-1]], axis=0),
                jnp.concatenate([south_mask[None], wet[:-1]], axis=0),
            ),
            (
                jnp.concatenate([center[1:], north[0][None]], axis=0),
                jnp.concatenate([wet[1:], north[1][None]], axis=0),
            ),
        )
        diffusion = jnp.zeros_like(center)
        for side_state, side_mask in sides:
            diffusion = diffusion + side_mask * (side_state - center)
        base[...] = (center + mixing[...][0][None, None, :] * diffusion).reshape(base.shape)
        total[...] = product

    @pl.when(step != 0)
    def _():
        total[...] += product

    @pl.when(step == pl.num_programs(0) - 1)
    def _():
        forcing = jnp.concatenate(
            [total[:, b * channels:(b + 1) * channels] for b in range(target_blocks)], axis=0
        )
        wet = mask[...].astype(jnp.float32)
        out[...] = (wet * (base[...] + forcing).reshape(out.shape)).astype(out.dtype)


def remap(table, place_of, source, tile_tgt, live, tile_weight, state, mask, mixing, lon, lat):
    tiles, block_rows, _ = tile_weight.shape
    channels = table.shape[1]
    cells = state.shape[0] * state.shape[1]
    per_step = max(d for d in range(1, 17) if tiles % d == 0)

    def block_spec(k):
        def index(i, place_of, source, tile_tgt, live):
            return (place_of[source[i * per_step + k]], 0)

        return pl.BlockSpec((block_rows, channels), index)

    def whole(array):
        return pl.BlockSpec(array.shape, lambda i, *_: (0,) * array.ndim)

    rest = (state, mask, mixing[None], lon, lat)
    return pl.pallas_call(
        functools.partial(remap_kernel, per_step),
        grid_spec=pltpu.PrefetchScalarGridSpec(
            num_scalar_prefetch=4,
            grid=(tiles // per_step,),
            in_specs=[
                pl.BlockSpec((per_step, block_rows, block_rows), lambda i, *_: (i, 0, 0)),
                *[block_spec(k) for k in range(per_step)],
                *[whole(a) for a in rest],
            ],
            out_specs=whole(state),
            scratch_shapes=[
                pltpu.VMEM((cells, channels), jnp.float32),
                pltpu.VMEM((block_rows, cells // block_rows * channels), jnp.float32),
            ],
        ),
        out_shape=jax.ShapeDtypeStruct(state.shape, state.dtype),
        compiler_params=pltpu.CompilerParams(
            dimension_semantics=("arbitrary",), vmem_limit_bytes=20 * 2**20
        ),
        name="remap_step",
    )(place_of, source, tile_tgt, live, tile_weight, *[table] * per_step, *rest)


def exchange(atm_fields, positions, tile_live, block_rows):
    channels = atm_fields.shape[1]
    block_count = atm_fields.shape[0] // block_rows
    devices = lax.axis_size("gx") * lax.axis_size("gy")
    per_peer = RECV_SLOTS // devices
    owners = positions // block_count
    local_slot = positions % block_count
    ordinal = jnp.arange(positions.shape[0], dtype=jnp.int32)
    active = ordinal < tile_live
    earlier = (
        (owners[:, None] == owners[None, :])
        & active[None, :]
        & (ordinal[None, :] < ordinal[:, None])
    )
    wanted_slot = owners * per_peer + jnp.sum(earlier.astype(jnp.int32), axis=1)
    slots_flat = jnp.arange(RECV_SLOTS, dtype=jnp.int32)
    matches = (wanted_slot[None, :] == slots_flat[:, None]) & active[None, :]
    asking = jnp.sum(jnp.where(matches, local_slot[None, :], 0), axis=1)
    wanted = lax.all_to_all(
        asking.reshape(devices, per_peer), ("gx", "gy"), split_axis=0, concat_axis=0, tiled=True
    ).reshape(RECV_SLOTS)
    outgoing = atm_fields.reshape(block_count, block_rows, channels)[wanted]
    outgoing = outgoing.reshape(devices, per_peer, block_rows, channels)
    arrived = lax.all_to_all(outgoing, ("gx", "gy"), split_axis=0, concat_axis=0, tiled=True)
    return arrived.reshape(RECV_SLOTS * block_rows, channels), jnp.where(active, wanted_slot, 0)


def swap_edges(lon, lat, sizes):
    n_gx, n_gy = sizes

    def shift(value, axis, size, by):
        return lax.ppermute(value, axis, [(i, (i + by) % size) for i in range(size)])

    lon_out = jnp.stack([shift(lon[1], "gx", n_gx, 1), shift(lon[0], "gx", n_gx, -1)])
    fold = lax.ppermute(lat[2], "gx", [(i, n_gx - 1 - i) for i in range(n_gx)])
    lat_out = jnp.stack([shift(lat[1], "gy", n_gy, 1), shift(lat[0], "gy", n_gy, -1), fold])
    return lon_out, lat_out


def local(
    atm_fields, atm_pos, tile_src, tile_tgt, tile_count, tile_weight, ocean_state, land_mask, mixing
):
    sizes = (lax.axis_size("gx"), lax.axis_size("gy"))
    block_rows = tile_weight.shape[1]
    mask = jnp.broadcast_to(land_mask.astype(jnp.bfloat16)[..., None], ocean_state.shape)
    both = jnp.stack([ocean_state, mask])
    lon = jnp.stack([both[:, :, 0], both[:, :, -1]])
    lat = jnp.stack([both[:, 0], both[:, -1], jnp.flip(both[:, -1], 1)])
    fits = atm_fields.size * 2 * sizes[0] * sizes[1] <= GATHER_BYTES
    if fits and sizes[0] == 4 and sizes[1] % 2 == 0:
        table, lon_in, lat_in, tile_weight = gather_all(atm_fields, lon, lat, tile_weight, sizes)
        place_of, source = atm_pos, tile_src
    else:
        table, place_of = exchange(atm_fields, atm_pos[tile_src], tile_count[0], block_rows)
        source = jnp.arange(tile_src.shape[0], dtype=jnp.int32)
        lon_in, lat_in = swap_edges(lon, lat, sizes)
    return remap(
        table, place_of, source, tile_tgt, tile_count, tile_weight, ocean_state, mask, mixing,
        lon_in, lat_in,
    )


def solution(mesh):
    in_specs = (
        P(("gx", "gy"), None),
        P(),
        P(("gx", "gy")),
        P(("gx", "gy")),
        P(("gx", "gy")),
        P(("gx", "gy"), None, None),
        P("gy", "gx", None),
        P("gy", "gx"),
        P(),
    )
    out_specs = P("gy", "gx", None)
    return jax.shard_map(local, mesh=mesh, in_specs=in_specs, out_specs=out_specs, check_vma=False)
```
